32 devices in a mesh: pp: 2 (over y), cp: 8 (over z, x), tp: 2 (over core).
Axes of the slice: x: 2, y: 2, z: 4, core: 2. Of those that a mesh axis runs over, the one named last changes fastest.
Arguments:
- queries: bfloat16 [2, 1024, 4096], P('pp', 'cp', 'tp'), may hold values from -4.5 to 4.5
- keys: bfloat16 [2, 1024, 256], P('pp', 'cp', 'tp'), may hold values from -4.5 to 4.5
- values: bfloat16 [2, 1024, 256], P('pp', 'cp', 'tp'), may hold values from -6 to 6
- out_weight: bfloat16 [4096, 16384], P('tp', 'cp'), may hold values from -1.5 to 1.5
- span_order: int32 [16], replicated, may hold values from 0 to 15, as said below
Outputs:
- handed: bfloat16 [2, 8, 128, 16384], P('pp', None, 'tp', 'cp')
The draws below stay inside these ranges and needn't reach their ends.
Inputs may be any that keep to these rules, and one draw needn't show every extreme that they name: `span_order`: the two stored blocks 2r and 2r + 1 are the sequence blocks j and 15 - j for some j, in either order; every sequence block appears once.
All inputs are finite; a program needn't handle non-finite values.
Results may differ from the reference program's by a relative error of at most 0.0095.
Values may be sent and summed in bfloat16 or wider, within the bound.
A program may use at most 128 MiB of HBM per device.

```python
import jax
import jax.numpy as jnp
from jax import lax

D = 16384
HEAD = 128
SPAN = 64
HEADS = 32
KVH = 2
TOKENS = 1024
N_PP = 2
N_CP = 8


def draw_keys(key, part):
    field = jnp.clip(jax.random.normal(jax.random.fold_in(key, 5), (N_PP, TOKENS, KVH * HEAD), jnp.float32), -4.5, 4.5)
    return field.astype(jnp.bfloat16)


def draw_queries(key, part):
    field = jnp.clip(jax.random.normal(jax.random.fold_in(key, 3), (N_PP, TOKENS, HEADS * HEAD), jnp.float32), -4.5, 4.5)
    return field.astype(jnp.bfloat16)


def draw_span_order(key, part):
    picked = jax.random.permutation(jax.random.fold_in(key, 21), N_CP)
    flipped = jax.random.randint(jax.random.fold_in(key, 22), (N_CP,), 0, 2)
    lower = jnp.where(flipped == 1, 2 * N_CP - 1 - picked, picked)
    upper = 2 * N_CP - 1 - lower
    return jnp.stack([lower, upper], axis=1).reshape(-1).astype(jnp.int32)


def block_levels(rng, extent, split, low, top_value):
    level = 1.0
    for axis_at, shards_of in split:
        draws = jax.random.uniform(jax.random.fold_in(jax.random.fold_in(rng, 6), axis_at), (shards_of,), jnp.float32, low / len(split), top_value / len(split))
        level = level * jnp.repeat(jnp.exp(draws), extent[axis_at] // shards_of).reshape((-1,) + (1,) * (len(extent) - 1 - axis_at))
    return level


def centred(stream_key, shape, deviation, reach, cuts=(), held_as=jnp.bfloat16):
    values = deviation * jax.random.normal(stream_key, shape, jnp.float32)
    if cuts:
        values = values * block_levels(stream_key, shape, cuts, -0.22, 0.18)
    return jnp.clip(values, -reach, reach).astype(held_as)


def setup_inputs(seed: int = 0) -> dict:
    key_of = jax.random.split(jax.random.key(seed), 6)
    return {
        "queries": draw_queries(jax.random.fold_in(key_of[5], 71), 0),
        "keys": draw_keys(jax.random.fold_in(key_of[5], 71), 0),
        "values": centred(key_of[2], (N_PP, TOKENS, KVH * HEAD), 1.0, 6.0, ((0, 2), (1, 8), (2, 2))),
        "out_weight": centred(key_of[3], (HEADS * HEAD, D), (max(HEADS * HEAD // 256, 1)) ** -0.5, 1.5, ((0, 2), (1, 8))),
        "span_order": draw_span_order(jax.random.fold_in(key_of[5], 71), 0),
    }


def reference(queries, keys, values, out_weight, span_order):
    offsets = jnp.arange(SPAN, dtype=jnp.int32)
    position = (span_order[:, None] * SPAN + offsets[None, :]).reshape(-1).astype(jnp.int32)
    allowed = position[None, :] <= position[:, None]
    group = HEADS // KVH
    scale = HEAD ** -0.5
    query_heads = queries.reshape(N_PP, TOKENS, HEADS, HEAD)
    key_heads = keys.reshape(N_PP, TOKENS, KVH, HEAD)
    value_heads = values.reshape(N_PP, TOKENS, KVH, HEAD)

    def single(index):
        section = index // HEADS
        head = index % HEADS
        query = query_heads[section, :, head]
        key_rows = key_heads[section, :, head // group]
        value_rows = value_heads[section, :, head // group]
        score = jnp.dot(query, key_rows.T, preferred_element_type=jnp.float32) * scale
        score = jnp.where(allowed, score, -1e30)
        summit = jnp.max(score, axis=-1, keepdims=True)
        weight = jnp.where(allowed, jnp.exp(score - summit), 0.0)
        total = jnp.sum(weight, axis=-1, keepdims=True)
        return jnp.dot(weight.astype(jnp.bfloat16), value_rows, preferred_element_type=jnp.float32) / total

    outputs = lax.map(single, jnp.arange(N_PP * HEADS, dtype=jnp.int32))
    attention = outputs.reshape(N_PP, HEADS, TOKENS, HEAD).transpose(0, 2, 1, 3)
    attention = attention.reshape(N_PP, TOKENS, HEADS * HEAD).astype(jnp.bfloat16)

    def project(section_rows):
        return jnp.dot(section_rows, out_weight, preferred_element_type=jnp.float32).astype(jnp.bfloat16)

    projected = lax.map(project, attention).reshape(N_PP, N_CP, 2 * SPAN, D)
    return jnp.roll(projected, 1, axis=0)
```

```python
import functools

import jax
import jax.numpy as jnp
from jax import lax
from jax.experimental import pallas as pl
from jax.experimental.pallas import tpu as pltpu
from jax.sharding import PartitionSpec as P

HEAD = 128
PARTS = 4
MESH = pl.DeviceIdType.MESH


def kernel(
    n_pp,
    n_cp,
    order_ref,
    q_ref,
    k_ref,
    v_ref,
    w_ref,
    out_ref,
    kv,
    qb,
    ga,
    wb,
    own,
    part,
    give,
    take,
    ob,
    mask,
    w_sem,
    out_sem,
    ys_sem,
    yr_sem,
    kvz_sem,
    kvx_sem,
    kvr_sem,
    up_sem,
    down_sem,
    x_sem,
    g_sem,
    ts_sem,
    tr_sem,
):
    pp, cp, tp = lax.axis_index("pp"), lax.axis_index("cp"), lax.axis_index("tp")
    line = n_cp // 2
    i, x = cp // 2, cp % 2
    rows = q_ref.shape[1]
    half = rows // 2
    width = qb.shape[2]
    tile = give.shape[3]
    heads = width // HEAD
    after, before = lax.rem(pp + 1, n_pp), lax.rem(pp + n_pp - 1, n_pp)
    right = (pp, i * 2 + 1 - x, tp)
    sibling = (pp, cp, 1 - tp)

    def remote(src, dst, send, recv, device):
        return pltpu.make_async_remote_copy(
            src_ref=src,
            dst_ref=dst,
            send_sem=send,
            recv_sem=recv,
            device_id=device,
            device_id_type=MESH,
        )

    load_w = pltpu.make_async_copy(w_ref, wb, w_sem)
    load_w.start()

    barrier = pltpu.get_barrier_semaphore()
    for device in ((after, cp, tp), (before, cp, tp), right, sibling):
        pl.semaphore_signal(barrier, inc=1, device_id=device, device_id_type=MESH)

    @pl.loop(0, line)
    def _(j):
        @pl.when(j != i)
        def _():
            pl.semaphore_signal(
                barrier, inc=1, device_id=(pp, j * 2 + x, tp), device_id_type=MESH
            )

    pl.semaphore_wait(barrier, 3 + line)

    shift = [
        remote(k_ref.at[0], kv.at[cp, 0], ys_sem.at[0], yr_sem.at[0], (after, cp, tp)),
        remote(v_ref.at[0], kv.at[cp, 1], ys_sem.at[1], yr_sem.at[1], (after, cp, tp)),
    ]
    for s in range(PARTS):
        shift.append(
            remote(
                q_ref.at[0, :, pl.ds(s * width, width)],
                qb.at[s],
                ys_sem.at[2 + s],
                yr_sem.at[2 + s],
                (after, cp, tp),
            )
        )
    for copy in shift:
        copy.start()
    shift[0].wait_recv()
    shift[1].wait_recv()

    def kv_line(c, j):
        return remote(kv.at[c], kv.at[c], kvz_sem.at[j], kvr_sem.at[c], (pp, j * 2 + x, tp))

    def kv_side(c):
        return remote(kv.at[c], kv.at[c], kvx_sem.at[c // 2], kvr_sem.at[c], right)

    def around(body):
        @pl.loop(1, line)
        def _(d):
            for j, inside in ((i - d, i - d >= 0), (i + d, i + d < line)):

                @pl.when(inside)
                def _():
                    body(j)

    around(lambda j: kv_line(cp, j).start())
    kv_side(cp).start()

    def pass_kv(j):
        kv_side(j * 2 + x).wait_recv()
        kv_side(j * 2 + x).start()

    around(pass_kv)

    @pl.loop(0, line)
    def _(j):
        kv_side(j * 2 + 1 - x).wait_recv()

    row = lax.broadcasted_iota(jnp.int32, (rows, 1), 0)
    query_pos = jnp.where(row < half, order_ref[2 * cp] * half, order_ref[2 * cp + 1] * half - half) + row
    for c in range(n_cp):
        col = lax.broadcasted_iota(jnp.int32, (1, rows), 1)
        key_pos = jnp.where(col < half, order_ref[2 * c] * half, order_ref[2 * c + 1] * half - half) + col
        mask[:, c * rows : (c + 1) * rows] = jnp.where(key_pos <= query_pos, 0.0, -1e30)

    def send_up(c, s):
        return remote(
            ga.at[c, s], ga.at[c, s], up_sem.at[c // 2, s], g_sem.at[c, s], (pp, cp + 2, tp)
        )

    def send_down(c, s):
        return remote(
            ga.at[c, s], ga.at[c, s], down_sem.at[c // 2, s], g_sem.at[c, s], (pp, cp - 2, tp)
        )

    def send_side(c, s):
        return remote(ga.at[c, s], ga.at[c, s], x_sem.at[c // 2, s], g_sem.at[c, s], right)

    scale = HEAD ** (-0.5)
    length = n_cp * rows
    for s in range(PARTS):
        shift[2 + s].wait_recv()

        @pl.loop(0, heads)
        def _(h):
            at = pl.ds(pl.multiple_of(h * HEAD, HEAD), HEAD)
            keys = kv[:, 0].reshape(length, HEAD)
            values = kv[:, 1].reshape(length, HEAD)
            score = lax.dot_general(
                qb[s, :, at], keys, (((1,), (1,)), ((), ())), preferred_element_type=jnp.float32
            )
            score = score * scale + mask[...]
            weight = jnp.exp(score - jnp.max(score, axis=1, keepdims=True))
            total = jnp.sum(weight, axis=1, keepdims=True)
            mixed = jnp.dot(weight.astype(jnp.bfloat16), values, preferred_element_type=jnp.float32)
            ga[cp, s, :, at] = (mixed / total).astype(jnp.bfloat16)

        @pl.when(i + 1 < line)
        def _():
            send_up(cp, s).start()

        @pl.when(i > 0)
        def _():
            send_down(cp, s).start()

        send_side(cp, s).start()

    load_w.wait()

    def swap(c, n):
        return remote(give.at[c, n], take.at[c, n], ts_sem.at[c, n], tr_sem.at[c, n], sibling)

    def columns(n):
        return pl.ds(pl.multiple_of(n * tile, tile), tile)

    def project(c, n):
        total = None
        for s in range(PARTS):
            term = jnp.dot(
                ga[c, s],
                wb[s * width : (s + 1) * width, columns(n)],
                preferred_element_type=jnp.float32,
            )
            total = term if total is None else total + term
        part[...] = total
        give[c, n] = part[pl.ds(pl.multiple_of((1 - tp) * half, half), half), :].astype(jnp.bfloat16)
        own[c, n] = part[pl.ds(pl.multiple_of(tp * half, half), half), :]
        swap(c, n).start()

    def finish(c, n):
        swap(c, n).wait_recv()
        ob[c, :, columns(n)] = (own[c, n] + take[c, n].astype(jnp.float32)).astype(jnp.bfloat16)

    def store(c):
        return pltpu.make_async_copy(ob.at[c], out_ref.at[0, c], out_sem.at[c])

    @pl.loop(PARTS, (line + 3) * PARTS)
    def _(step):
        d, s = step // PARTS, step % PARTS

        @pl.when((d < line) & (i - d >= 0))
        def _():
            c = cp - 2 * d
            send_side(c, s).wait_recv()

            @pl.when(i + 1 < line)
            def _():
                send_up(c, s).start()

            send_side(c, s).start()

        @pl.when((d < line) & (i + d < line))
        def _():
            c = cp + 2 * d
            send_side(c, s).wait_recv()

            @pl.when(i > 0)
            def _():
                send_down(c, s).start()

            send_side(c, s).start()

        @pl.loop(0, 4)
        def _(k):
            side = k // 2
            sign = 1 - 2 * (k % 2)

            def item(lag):
                far = d - lag - side
                j = i + sign * far
                c = j * 2 + (x + side) % 2
                fine = (far >= 0) & (far < line) & (j >= 0) & (j < line)
                return c, fine & ((far > 0) | (sign > 0))

            c, fine = item(1)

            @pl.when(fine)
            def _():
                @pl.when((side == 1) & (s == 0))
                def _():
                    for r in range(PARTS):
                        send_side(c, r).wait_recv()

                project(c, s)

            e, done = item(2)

            @pl.when(done)
            def _():
                finish(e, s)

                @pl.when(s == PARTS - 1)
                def _():
                    store(e).start()

    for copy in shift:
        copy.wait_send()
    around(lambda j: kv_line(cp, j).wait_send())

    @pl.loop(0, line)
    def _(j):
        c = j * 2 + x
        kv_side(c).wait_send()
        for s in range(PARTS):
            send_side(c, s).wait_send()

            @pl.when((j <= i) & (i + 1 < line))
            def _():
                send_up(c, s).wait_send()

            @pl.when((j >= i) & (i > 0))
            def _():
                send_down(c, s).wait_send()

    @pl.loop(0, n_cp)
    def _(c):
        for n in range(PARTS):
            swap(c, n).wait_send()
        store(c).wait()


def on_device(n_pp, n_cp, queries, keys, values, out_weight, span_order):
    rows = queries.shape[1]
    half = rows // 2
    depth, wide = out_weight.shape
    width, tile = depth // PARTS, wide // PARTS
    line = n_cp // 2
    vmem = pl.BlockSpec(memory_space=pltpu.VMEM)
    hbm = pl.BlockSpec(memory_space=pl.ANY)
    dma = pltpu.SemaphoreType.DMA
    return pl.pallas_call(
        functools.partial(kernel, n_pp, n_cp),
        out_shape=jax.ShapeDtypeStruct((1, n_cp, half, wide), jnp.bfloat16),
        in_specs=[pl.BlockSpec(memory_space=pltpu.SMEM), vmem, vmem, vmem, hbm],
        out_specs=hbm,
        scratch_shapes=[
            pltpu.VMEM((n_cp, 2, rows, HEAD), jnp.bfloat16),
            pltpu.VMEM((PARTS, rows, width), jnp.bfloat16),
            pltpu.VMEM((n_cp, PARTS, rows, width), jnp.bfloat16),
            pltpu.VMEM((depth, wide), jnp.bfloat16),
            pltpu.VMEM((n_cp, PARTS, half, tile), jnp.float32),
            pltpu.VMEM((rows, tile), jnp.float32),
            pltpu.VMEM((n_cp, PARTS, half, tile), jnp.bfloat16),
            pltpu.VMEM((n_cp, PARTS, half, tile), jnp.bfloat16),
            pltpu.VMEM((n_cp, half, wide), jnp.bfloat16),
            pltpu.VMEM((rows, n_cp * rows), jnp.float32),
            dma,
            dma((n_cp,)),
            dma((2 + PARTS,)),
            dma((2 + PARTS,)),
            dma((line,)),
            dma((line,)),
            dma((n_cp,)),
            dma((line, PARTS)),
            dma((line, PARTS)),
            dma((line, PARTS)),
            dma((n_cp, PARTS)),
            dma((n_cp, PARTS)),
            dma((n_cp, PARTS)),
        ],
        compiler_params=pltpu.CompilerParams(
            collective_id=0, has_side_effects=True, vmem_limit_bytes=60000 * 1024
        ),
    )(span_order, queries, keys, values, out_weight)


def solution(mesh):
    placed = (P("pp", "cp", "tp"), P("pp", "cp", "tp"), P("pp", "cp", "tp"), P("tp", "cp"), P())
    return jax.shard_map(
        functools.partial(on_device, mesh.shape["pp"], mesh.shape["cp"]),
        mesh=mesh,
        in_specs=placed,
        out_specs=P("pp", None, "tp", "cp"),
        check_vma=False,
    )
```

```python
import functools

import jax
import jax.numpy as jnp
from jax import lax
from jax.experimental import pallas as pl
from jax.experimental.pallas import tpu as pltpu
from jax.sharding import PartitionSpec as P

HEAD = 128
PARTS = 8
RAW = 0
RAW_AT = 0
MESH = pl.DeviceIdType.MESH


def kernel(
    n_pp,
    n_cp,
    order_ref,
    q_ref,
    k_ref,
    v_ref,
    w_ref,
    out_ref,
    kv,
    qb,
    ga,
    wb,
    own,
    part,
    give,
    take,
    ob,
    raw,
    key_pos,
    w_sem,
    out_sem,
    ys_sem,
    yr_sem,
    kvz_sem,
    kvx_sem,
    kvr_sem,
    up_sem,
    down_sem,
    x_sem,
    g_sem,
    ts_sem,
    tr_sem,
):
    pp, cp, tp = lax.axis_index("pp"), lax.axis_index("cp"), lax.axis_index("tp")
    line = n_cp // 2
    i, x = cp // 2, cp % 2
    rows = q_ref.shape[1]
    half = rows // 2
    width = qb.shape[2]
    tile = give.shape[3]
    heads = width // HEAD
    after, before = lax.rem(pp + 1, n_pp), lax.rem(pp + n_pp - 1, n_pp)
    right = (pp, i * 2 + 1 - x, tp)
    sibling = (pp, cp, 1 - tp)

    def remote(src, dst, send, recv, device):
        return pltpu.make_async_remote_copy(
            src_ref=src,
            dst_ref=dst,
            send_sem=send,
            recv_sem=recv,
            device_id=device,
            device_id_type=MESH,
        )

    load_w = pltpu.make_async_copy(w_ref, wb, w_sem)
    load_w.start()

    barrier = pltpu.get_barrier_semaphore()
    for device in ((after, cp, tp), (before, cp, tp), right, sibling):
        pl.semaphore_signal(barrier, inc=1, device_id=device, device_id_type=MESH)

    @pl.loop(0, line)
    def _(j):
        @pl.when(j != i)
        def _():
            pl.semaphore_signal(
                barrier, inc=1, device_id=(pp, j * 2 + x, tp), device_id_type=MESH
            )

    pl.semaphore_wait(barrier, 3 + line)

    shift = [
        remote(k_ref.at[0], kv.at[cp, 0], ys_sem.at[0], yr_sem.at[0], (after, cp, tp)),
        remote(v_ref.at[0], kv.at[cp, 1], ys_sem.at[1], yr_sem.at[1], (after, cp, tp)),
    ]
    for s in range(PARTS):
        shift.append(
            remote(
                q_ref.at[0, :, pl.ds(s * width, width)],
                ga.at[cp, s] if s < RAW else qb.at[s],
                ys_sem.at[2 + s],
                yr_sem.at[2 + s],
                (after, cp, tp),
            )
        )
    for copy in shift:
        copy.start()
    shift[0].wait_recv()
    shift[1].wait_recv()

    def kv_line(c, j):
        return remote(kv.at[c], kv.at[c], kvz_sem.at[j], kvr_sem.at[c], (pp, j * 2 + x, tp))

    def kv_side(c):
        return remote(kv.at[c], kv.at[c], kvx_sem.at[c // 2], kvr_sem.at[c], right)

    def around(body):
        @pl.loop(1, line)
        def _(d):
            for j, inside in ((i - d, i - d >= 0), (i + d, i + d < line)):

                @pl.when(inside)
                def _():
                    body(j)

    around(lambda j: kv_line(cp, j).start())
    kv_side(cp).start()

    def pass_kv(j):
        kv_side(j * 2 + x).wait_recv()
        kv_side(j * 2 + x).start()

    def send_up(c, s):
        return remote(
            ga.at[c, s], ga.at[c, s], up_sem.at[c // 2, s], g_sem.at[c, s], (pp, cp + 2, tp)
        )

    def send_down(c, s):
        return remote(
            ga.at[c, s], ga.at[c, s], down_sem.at[c // 2, s], g_sem.at[c, s], (pp, cp - 2, tp)
        )

    def send_side(c, s):
        return remote(ga.at[c, s], ga.at[c, s], x_sem.at[c // 2, s], g_sem.at[c, s], right)

    def send_own(s):
        @pl.when(i + 1 < line)
        def _():
            send_up(cp, s).start()

        @pl.when(i > 0)
        def _():
            send_down(cp, s).start()

        send_side(cp, s).start()

    def relay(d, s):
        @pl.when((d < line) & (i - d >= 0))
        def _():
            c = cp - 2 * d
            send_side(c, s).wait_recv()

            @pl.when(i + 1 < line)
            def _():
                send_up(c, s).start()

            send_side(c, s).start()

        @pl.when((d < line) & (i + d < line))
        def _():
            c = cp + 2 * d
            send_side(c, s).wait_recv()

            @pl.when(i > 0)
            def _():
                send_down(c, s).start()

            send_side(c, s).start()

    for s in range(RAW):
        shift[2 + s].wait_recv()
        send_own(s)

    around(pass_kv)
    for s in range(RAW):
        relay(1, s)

    @pl.loop(0, line)
    def _(j):
        kv_side(j * 2 + 1 - x).wait_recv()

    def position(c, iota):
        first, second = order_ref[2 * c] * half, order_ref[2 * c + 1] * half - half
        return jnp.where(iota < half, first, second) + iota

    for c in range(n_cp):
        col = lax.broadcasted_iota(jnp.int32, (1, rows), 1)
        key_pos[:, c * rows : (c + 1) * rows] = position(c, col)

    scale = HEAD ** (-0.5)
    length = n_cp * rows

    def attend(c, source, target):
        keys = kv[:, 0].reshape(length, HEAD)
        values = kv[:, 1].reshape(length, HEAD)
        query_pos = position(c, lax.broadcasted_iota(jnp.int32, (rows, 1), 0))
        allowed = jnp.where(key_pos[...] <= query_pos, 0.0, -1e30)
        query = source[...]
        query = jnp.concatenate([query[:, h * HEAD : (h + 1) * HEAD] for h in range(heads)], axis=0)
        score = lax.dot_general(
            query, keys, (((1,), (1,)), ((), ())), preferred_element_type=jnp.float32
        )
        for h in range(heads):
            piece = score[h * rows : (h + 1) * rows] * scale + allowed
            weight = jnp.exp(piece - jnp.max(piece, axis=1, keepdims=True))
            total = jnp.sum(weight, axis=1, keepdims=True)
            mixed = jnp.dot(
                weight.astype(jnp.bfloat16), values, preferred_element_type=jnp.float32
            )
            target[:, h * HEAD : (h + 1) * HEAD] = (mixed / total).astype(jnp.bfloat16)

    for s in range(RAW, PARTS):
        shift[2 + s].wait_recv()
        attend(cp, qb.at[s], ga.at[cp, s])
        send_own(s)
        for r in range(RAW):
            relay(2 + s - RAW, r)

    @pl.loop(line if RAW == 0 else 2 + PARTS - RAW, line)
    def _(d):
        for r in range(RAW):
            relay(d, r)

    load_w.wait()

    def swap(c, n):
        return remote(give.at[c, n], take.at[c, n], ts_sem.at[c, n], tr_sem.at[c, n], sibling)

    def columns(n):
        return pl.ds(pl.multiple_of(n * tile, tile), tile)

    def project(c, n):
        total = None
        for s in range(PARTS):
            term = jnp.dot(
                raw[c, s] if s < RAW else ga[c, s],
                wb[s * width : (s + 1) * width, columns(n)],
                preferred_element_type=jnp.float32,
            )
            total = term if total is None else total + term
        part[...] = total
        give[c, n] = part[pl.ds(pl.multiple_of((1 - tp) * half, half), half), :].astype(jnp.bfloat16)
        own[c, n] = part[pl.ds(pl.multiple_of(tp * half, half), half), :]
        swap(c, n).start()

    def finish(c, n):
        swap(c, n).wait_recv()
        ob[c, :, columns(n)] = (own[c, n] + take[c, n].astype(jnp.float32)).astype(jnp.bfloat16)

    def store(c):
        return pltpu.make_async_copy(ob.at[c], out_ref.at[0, c], out_sem.at[c])

    @pl.loop(PARTS, (line + 4) * PARTS)
    def _(step):
        d, s = step // PARTS, step % PARTS

        @pl.when(s >= RAW)
        def _():
            relay(d, s)

        @pl.loop(0, 4)
        def _(k):
            side = k // 2
            sign = 1 - 2 * (k % 2)

            def item(lag):
                far = d - lag - side
                j = i + sign * far
                c = j * 2 + (x + side) % 2
                fine = (far >= 0) & (far < line) & (j >= 0) & (j < line)
                return c, fine & ((far > 0) | (sign > 0))

            b, here = item(1)

            @pl.when(here)
            def _():
                for r in range(RAW):

                    @pl.when(s == RAW_AT)
                    def _():
                        @pl.when(side == 1)
                        def _():
                            send_side(b, r).wait_recv()

                        attend(b, ga.at[b, r], raw.at[b, r])

            c, fine = item(2)

            @pl.when(fine)
            def _():
                @pl.when((side == 1) & (s == 0))
                def _():
                    for r in range(RAW, PARTS):
                        send_side(c, r).wait_recv()

                project(c, s)

            e, done = item(3)

            @pl.when(done)
            def _():
                finish(e, s)

                @pl.when(s == PARTS - 1)
                def _():
                    store(e).start()

    for copy in shift:
        copy.wait_send()
    around(lambda j: kv_line(cp, j).wait_send())

    @pl.loop(0, line)
    def _(j):
        c = j * 2 + x
        kv_side(c).wait_send()
        for s in range(PARTS):
            send_side(c, s).wait_send()

            @pl.when((j <= i) & (i + 1 < line))
            def _():
                send_up(c, s).wait_send()

            @pl.when((j >= i) & (i > 0))
            def _():
                send_down(c, s).wait_send()

    @pl.loop(0, n_cp)
    def _(c):
        for n in range(PARTS):
            swap(c, n).wait_send()
        store(c).wait()


def on_device(n_pp, n_cp, queries, keys, values, out_weight, span_order):
    rows = queries.shape[1]
    half = rows // 2
    depth, wide = out_weight.shape
    width, tile = depth // PARTS, wide // PARTS
    line = n_cp // 2
    vmem = pl.BlockSpec(memory_space=pltpu.VMEM)
    hbm = pl.BlockSpec(memory_space=pl.ANY)
    dma = pltpu.SemaphoreType.DMA
    return pl.pallas_call(
        functools.partial(kernel, n_pp, n_cp),
        out_shape=jax.ShapeDtypeStruct((1, n_cp, half, wide), jnp.bfloat16),
        in_specs=[pl.BlockSpec(memory_space=pltpu.SMEM), vmem, vmem, vmem, hbm],
        out_specs=hbm,
        scratch_shapes=[
            pltpu.VMEM((n_cp, 2, rows, HEAD), jnp.bfloat16),
            pltpu.VMEM((PARTS, rows, width), jnp.bfloat16),
            pltpu.VMEM((n_cp, PARTS, rows, width), jnp.bfloat16),
            pltpu.VMEM((depth, wide), jnp.bfloat16),
            pltpu.VMEM((n_cp, PARTS, half, tile), jnp.float32),
            pltpu.VMEM((rows, tile), jnp.float32),
            pltpu.VMEM((n_cp, PARTS, half, tile), jnp.bfloat16),
            pltpu.VMEM((n_cp, PARTS, half, tile), jnp.bfloat16),
            pltpu.VMEM((n_cp, half, wide), jnp.bfloat16),
            pltpu.VMEM((n_cp, max(RAW, 1), rows, width), jnp.bfloat16),
            pltpu.VMEM((1, n_cp * rows), jnp.int32),
            dma,
            dma((n_cp,)),
            dma((2 + PARTS,)),
            dma((2 + PARTS,)),
            dma((line,)),
            dma((line,)),
            dma((n_cp,)),
            dma((line, PARTS)),
            dma((line, PARTS)),
            dma((line, PARTS)),
            dma((n_cp, PARTS)),
            dma((n_cp, PARTS)),
            dma((n_cp, PARTS)),
        ],
        compiler_params=pltpu.CompilerParams(
            collective_id=0, has_side_effects=True, vmem_limit_bytes=60000 * 1024
        ),
    )(span_order, queries, keys, values, out_weight)


def solution(mesh):
    placed = (P("pp", "cp", "tp"), P("pp", "cp", "tp"), P("pp", "cp", "tp"), P("tp", "cp"), P())
    return jax.shard_map(
        functools.partial(on_device, mesh.shape["pp"], mesh.shape["cp"]),
        mesh=mesh,
        in_specs=placed,
        out_specs=P("pp", None, "tp", "cp"),
        check_vma=False,
    )
```
